32 devices in a mesh: band: 8 (over z, y), sub: 4 (over x, core).
Axes of the slice: x: 2, y: 2, z: 4, core: 2. Of those that a mesh axis runs over, the one named last changes fastest.
Arguments:
- grid_x: bfloat16 [227, 16384], P(None, ('band', 'sub')), may hold values from -6 to 6
- mesh_in: bfloat16 [2048, 512], P(('band', 'sub')), may hold values from -6 to 6
- w_embed: bfloat16 [227, 512], replicated, may hold values from -0.375 to 0.375
- w_src: bfloat16 [512, 512], replicated, may hold values from -0.25 to 0.25
- w_dst: bfloat16 [512, 512], replicated, may hold values from -0.25 to 0.25
- w_edge: bfloat16 [512, 512], replicated, may hold values from -0.25 to 0.25
- w_proc: bfloat16 [512, 512], replicated, may hold values from -0.25 to 0.25
- w_recv: bfloat16 [512, 512], replicated, may hold values from -0.25 to 0.25
- g2m_src: int32 [2048, 40], P(('band', 'sub')), may hold values from 0 to 16383, as said below
- mesh_src: int32 [2048, 6], P(('band', 'sub')), may hold values from 0 to 2047, as said below
- cotangent: bfloat16 [2048, 512], P(('band', 'sub')), may hold values from -6 to 6
Outputs:
- mesh_out: bfloat16 [2048, 512], P(('band', 'sub'))
- grid_grad: float32 [227, 16384], P(None, ('band', 'sub'))
- src_grad: float32 [512, 512], replicated
- edge_grad: float32 [512, 512], replicated
The draws below stay inside these ranges and needn't reach their ends.
Inputs may be any that keep to these rules, and one draw needn't show every extreme that they name: Grid node g belongs to band g // (512 * 4), mesh node m to band m // (64 * 4); g2m_src[m, k] lies in the band of mesh node m, or among the 512 grid nodes of an adjacent band that stand next to that band in index order. mesh_src[m, j] lies in the band of mesh node m, or among the 64 mesh nodes of an adjacent band that stand next to that band in index order.
All inputs are finite; a program needn't handle non-finite values.
Results may differ from the reference program's by a relative error of at most 0.015.
Values may be sent and summed in bfloat16 or wider, within the bound.
A program may use at most 128 MiB of HBM per device.

```python
import math
import jax
import jax.numpy as jnp
from jax import lax

LATENT = 512
CHANNELS = 227
GRID_DEV = 512
MESH_DEV = 64
ENC_EDGES = 40
MESH_EDGES = 6
GRID = 16384
MESH = 2048
N_BAND = 8
N_SUB = 4


def band_sources(key, count, edges, node_dev, source_dev):
    node_band = jnp.arange(count, dtype=jnp.int32) // (node_dev * N_SUB)
    width = source_dev * N_SUB
    total = width * N_BAND
    lowest = jnp.maximum(node_band * width - source_dev, 0)
    highest = jnp.minimum((node_band + 1) * width + source_dev, total)
    return jax.random.randint(key, (count, edges), lowest[:, None], highest[:, None], dtype=jnp.int32)


def draw_g2m_src(key, part):
    return band_sources(jax.random.fold_in(key, 11), MESH, ENC_EDGES, MESH_DEV, GRID_DEV)


def draw_mesh_src(key, part):
    return band_sources(jax.random.fold_in(key, 23), MESH, MESH_EDGES, MESH_DEV, MESH_DEV)


def block_scale(own_key, extent, shards, low, largest):
    gain, own = 1.0, jax.random.fold_in(own_key, 6)
    for position, blocks in shards:
        draws = jnp.exp(jax.random.uniform(jax.random.fold_in(own, position), (blocks,), jnp.float32, low / len(shards), largest / len(shards)))
        gain = gain * jnp.repeat(draws, extent[position] // blocks).reshape([-1 if axis == position else 1 for axis in range(len(extent))])
    return gain


def noise(own_key, shape, scale, reach, shards=(), kind=jnp.bfloat16):
    values = jax.random.normal(own_key, shape, jnp.float32) * scale
    if len(shards) > 0:
        values = block_scale(own_key, shape, shards, -0.22, 0.18) * values
    return jnp.clip(values, min=-reach, max=reach).astype(kind)


def setup_inputs(seed: int = 0) -> dict:
    arg_keys = jax.random.split(jax.random.key(seed), 12)
    return {
        "grid_x": noise(arg_keys[0], (CHANNELS, GRID), 1.0, 6.0, ((1, 32),)),
        "mesh_in": noise(arg_keys[1], (MESH, LATENT), 1.0, 6.0, ((0, 32),)),
        "w_embed": noise(arg_keys[2], (CHANNELS, LATENT), CHANNELS ** -0.5, 0.375),
        "w_src": noise(arg_keys[3], (LATENT, LATENT), LATENT ** -0.5, 0.25),
        "w_dst": noise(arg_keys[4], (LATENT, LATENT), LATENT ** -0.5, 0.25),
        "w_edge": noise(arg_keys[5], (LATENT, LATENT), LATENT ** -0.5, 0.25),
        "w_proc": noise(arg_keys[6], (LATENT, LATENT), LATENT ** -0.5, 0.25),
        "w_recv": noise(arg_keys[7], (LATENT, LATENT), LATENT ** -0.5, 0.25),
        "g2m_src": draw_g2m_src(jax.random.fold_in(arg_keys[11], 71), 0),
        "mesh_src": draw_mesh_src(jax.random.fold_in(arg_keys[11], 71), 0),
        "cotangent": noise(arg_keys[10], (MESH, LATENT), 1.0, 6.0, ((0, 32),)),
    }


EPSILON = 1e-05

def silu_slope(value):
    sigma = jax.nn.sigmoid(value)
    return sigma * (1.0 + value * (1.0 - sigma))

def normalize(value):
    centred = value - lax.optimization_barrier(jnp.mean(value, axis=-1, keepdims=True))
    spread = jnp.sqrt(lax.optimization_barrier(jnp.mean(centred * centred, axis=-1, keepdims=True)) + EPSILON)
    return (centred / spread, spread)

def times_transpose(left, right):
    return lax.dot_general(left, right, (((1,), (1,)), ((), ())), preferred_element_type=jnp.float32)

def first_contract(left, right):
    return lax.dot_general(left, right, (((0,), (0,)), ((), ())), preferred_element_type=jnp.float32)

def encoder_edges(projected, indices, dest_term, w_edge):
    rows = dest_term.shape[0]
    before = jnp.take(projected, indices, axis=0).astype(jnp.float32)
    before = (before.reshape(rows, ENC_EDGES, LATENT) + dest_term[:, None, :]).reshape(rows * ENC_EDGES, LATENT)
    active = jax.nn.silu(before).astype(jnp.bfloat16)
    normed, spread = normalize(jnp.dot(active, w_edge, preferred_element_type=jnp.float32))
    return (before, active, normed, spread)

def reference(grid_x, mesh_in, w_embed, w_src, w_dst, w_edge, w_proc, w_recv, g2m_src, mesh_src, cotangent):
    blocks = MESH // MESH_DEV
    hidden_pre = first_contract(grid_x, w_embed)
    hidden_grid = jax.nn.silu(hidden_pre).astype(jnp.bfloat16)
    projected = jnp.dot(hidden_grid, w_src, preferred_element_type=jnp.float32).astype(jnp.bfloat16)
    dest_term = jnp.dot(mesh_in, w_dst, preferred_element_type=jnp.float32)
    index_blocks = g2m_src.reshape(blocks, MESH_DEV * ENC_EDGES)
    dest_blocks = dest_term.reshape(blocks, MESH_DEV, LATENT)

    def encode(pair):
        before, active, normed, spread = encoder_edges(projected, pair[0], pair[1], w_edge)
        return lax.optimization_barrier(jnp.sum(normed.reshape(MESH_DEV, ENC_EDGES, LATENT), axis=1))
    encoded = lax.map(encode, (index_blocks, dest_blocks)).reshape(MESH, LATENT)
    hidden_mesh = (mesh_in.astype(jnp.float32) + encoded / math.sqrt(ENC_EDGES)).astype(jnp.bfloat16)
    query = jnp.dot(hidden_mesh, w_proc, preferred_element_type=jnp.float32).astype(jnp.bfloat16)
    receiver = jnp.dot(hidden_mesh, w_recv, preferred_element_type=jnp.float32)
    flat_mesh = mesh_src.reshape(-1)
    mesh_before = jnp.take(query, flat_mesh, axis=0).astype(jnp.float32).reshape(MESH, MESH_EDGES, LATENT)
    mesh_before = mesh_before + receiver[:, None, :]
    summed = lax.optimization_barrier(jnp.sum(jax.nn.silu(mesh_before), axis=1))
    mesh_out = (hidden_mesh.astype(jnp.float32) + summed / math.sqrt(MESH_EDGES)).astype(jnp.bfloat16)
    upstream = cotangent.astype(jnp.float32)
    mesh_slope = (upstream / math.sqrt(MESH_EDGES))[:, None, :] * silu_slope(mesh_before)
    receiver_grad = lax.optimization_barrier(jnp.sum(mesh_slope, axis=1))
    query_grad = jnp.zeros((MESH, LATENT), jnp.float32).at[flat_mesh].add(mesh_slope.reshape(-1, LATENT))
    mesh_grad = upstream + times_transpose(query_grad.astype(jnp.bfloat16), w_proc)
    mesh_grad = mesh_grad + times_transpose(receiver_grad.astype(jnp.bfloat16), w_recv)
    grad_blocks = (mesh_grad / math.sqrt(ENC_EDGES)).reshape(blocks, MESH_DEV, LATENT)

    def backward(carry, triple):
        projected_grad, edge_total = carry
        indices, dest, upper = triple
        before, active, normed, spread = encoder_edges(projected, indices, dest, w_edge)
        incoming = jnp.broadcast_to(upper[:, None, :], (MESH_DEV, ENC_EDGES, LATENT)).reshape(-1, LATENT)
        centred_grad = incoming - lax.optimization_barrier(jnp.mean(incoming, axis=-1, keepdims=True))
        centred_grad = centred_grad - normed * lax.optimization_barrier(jnp.mean(incoming * normed, axis=-1, keepdims=True))
        norm_grad = (centred_grad / spread).astype(jnp.bfloat16)
        edge_total = edge_total + first_contract(active, norm_grad)
        before_grad = times_transpose(norm_grad, w_edge) * silu_slope(before)
        projected_grad = projected_grad.at[indices].add(before_grad)
        return ((projected_grad, edge_total), None)
    start = (jnp.zeros((GRID, LATENT), jnp.float32), jnp.zeros((LATENT, LATENT), jnp.float32))
    (projected_grad, edge_grad), _ = lax.scan(backward, start, (index_blocks, dest_blocks, grad_blocks))
    projected_low = projected_grad.astype(jnp.bfloat16)
    src_grad = first_contract(hidden_grid, projected_low)
    hidden_grad = (times_transpose(projected_low, w_src) * silu_slope(hidden_pre)).astype(jnp.bfloat16)
    grid_grad = times_transpose(w_embed, hidden_grad)
    return (mesh_out, grid_grad, src_grad, edge_grad)
```

```python
import functools
import math

import jax
import jax.numpy as jnp
from jax import lax
from jax.experimental import pallas as pl
from jax.experimental.pallas import tpu as pltpu
from jax.sharding import PartitionSpec as P

EPSILON = 1e-05
F32 = jnp.float32
BF16 = jnp.bfloat16
LANES = 128
INNER = 2
VMEM = pl.BlockSpec(memory_space=pltpu.VMEM)
SMEM = pl.BlockSpec(memory_space=pltpu.SMEM)
ANY = pl.BlockSpec(memory_space=pl.ANY)


def contract(left, right, left_dim, right_dim):
    return lax.dot_general(
        left, right, (((left_dim,), (right_dim,)), ((), ())), preferred_element_type=F32
    )


def silu_pair(value):
    sigma = 0.5 * jnp.tanh(0.5 * value) + 0.5
    active = value * sigma
    return active, sigma + active * (1.0 - sigma)


def remote(src, dst, send, recv, device):
    return pltpu.make_async_remote_copy(
        src_ref=src,
        dst_ref=dst,
        send_sem=send,
        recv_sem=recv,
        device_id=device,
        device_id_type=pl.DeviceIdType.MESH,
    )


def greet(barrier, device):
    pl.semaphore_signal(barrier, inc=1, device_id=device, device_id_type=pl.DeviceIdType.MESH)


class Place:
    def __init__(self, bands, subs):
        self.bands, self.subs = bands, subs
        self.band, self.me = lax.axis_index("band"), lax.axis_index("sub")
        self.core = lax.rem(self.me, 2)
        self.chip = self.me // 2
        self.partner = self.me + 1 - 2 * self.core
        self.chips = subs // 2
        self.outer, self.inner = self.band // INNER, lax.rem(self.band, INNER)
        self.outers = bands // INNER


def entry_barrier(at):
    barrier = pltpu.get_barrier_semaphore()
    for step in range(1, at.subs):
        greet(barrier, (at.band, lax.rem(at.me + step, at.subs)))

    @pl.when(at.band > 0)
    def _():
        for other in range(at.subs):
            greet(barrier, (at.band - 1, other))

    @pl.when(at.band < at.bands - 1)
    def _():
        for other in range(at.subs):
            greet(barrier, (at.band + 1, other))

    for i in range(1, at.outers):
        greet(barrier, (lax.rem(at.outer + i, at.outers) * INNER + at.inner, at.me))
    sides = jnp.minimum(at.band, 1) + jnp.minimum(at.bands - 1 - at.band, 1)
    pl.semaphore_wait(barrier, at.subs - 1 + at.subs * sides + at.outers - 1)


class Fetch:
    def __init__(self, at, src, o_ref, send, recv):
        self.at, self.src, self.o_ref, self.send, self.recv = at, src, o_ref, send, recv
        chips = at.chips
        self.across = [
            self.push(src, 1 + at.me, at.band, 2 * lax.rem(at.chip + k, chips) + at.core, k - 1)
            for k in range(1, chips)
        ]
        self.pair = self.push(src, 1 + at.me, at.band, at.partner, chips - 1)
        self.rising = (at.me == at.subs - 1) & (at.band < at.bands - 1)
        self.falling = (at.me == 0) & (at.band > 0)
        self.direct_below = (at.core == 1) & (at.band > 0)
        self.direct_above = (at.core == 0) & (at.band < at.bands - 1)
        top = at.subs + 1
        self.relay_below = self.push(o_ref.at[0], 0, at.band, at.partner, 4 * chips - 1)
        self.relay_above = self.push(o_ref.at[top], top, at.band, at.partner, 4 * chips)
        self.relays = []
        for k in range(1, chips):
            slot = self.near(k)
            self.relays.append(
                self.push(o_ref.at[slot], slot, at.band, at.partner, 3 * chips + k - 1)
            )

    def push(self, src, slot, b, s, index):
        return remote(src, self.o_ref.at[slot], self.send.at[index], self.recv.at[slot], (b, s))

    def near(self, k):
        at = self.at
        return 1 + 2 * lax.rem(at.chip + at.chips - k, at.chips) + at.core

    def up(self, k):
        at = self.at
        return self.push(self.src, 0, at.band + 1, 2 * k + 1, at.chips + k)

    def down(self, k):
        at = self.at
        return self.push(self.src, at.subs + 1, at.band - 1, 2 * k, 2 * at.chips + k)

    def arrived(self, slot):
        self.push(self.src, slot, self.at.band, self.at.partner, 0).wait_recv()

    def start(self):
        for copy in self.across:
            copy.start()
        self.pair.start()

        @pl.when(self.rising)
        def _():
            for k in range(self.at.chips):
                self.up(k).start()

        @pl.when(self.falling)
        def _():
            for k in range(self.at.chips):
                self.down(k).start()

    def clear(self):
        at = self.at
        block, kind = self.o_ref.shape[1:], self.o_ref.dtype

        @pl.when(at.band == 0)
        def _():
            self.o_ref[0] = jnp.zeros(block, kind)

        @pl.when(at.band == at.bands - 1)
        def _():
            self.o_ref[at.subs + 1] = jnp.zeros(block, kind)

    def wait_partner(self):
        self.arrived(1 + self.at.partner)

    def wait_near(self, k):
        self.arrived(self.near(k))
        self.relays[k - 1].start()

    def wait_far(self, k):
        self.arrived(self.near(k) + 1 - 2 * self.at.core)

    def wait_border(self):
        @pl.when(self.direct_below)
        def _():
            self.arrived(0)
            self.relay_below.start()

        @pl.when(self.direct_above)
        def _():
            self.arrived(self.at.subs + 1)
            self.relay_above.start()

    def wait_other_border(self):
        at = self.at

        @pl.when((at.core == 0) & (at.band > 0))
        def _():
            self.arrived(0)

        @pl.when((at.core == 1) & (at.band < at.bands - 1))
        def _():
            self.arrived(at.subs + 1)

    def finish(self):
        for copy in self.across + [self.pair] + self.relays:
            copy.wait_send()

        @pl.when(self.rising)
        def _():
            for k in range(self.at.chips):
                self.up(k).wait_send()

        @pl.when(self.falling)
        def _():
            for k in range(self.at.chips):
                self.down(k).wait_send()

        @pl.when(self.direct_below)
        def _():
            self.relay_below.wait_send()

        @pl.when(self.direct_above)
        def _():
            self.relay_above.wait_send()


def fetch_scratch(at_chips, subs):
    dma = pltpu.SemaphoreType.DMA
    return [dma((4 * at_chips + 1,)), dma((subs + 2,))]


class Return:
    def __init__(self, at, g_ref, pairbuf, stage, far, edge, send1, recv1, send2, far_sem, edge_sem):
        self.at, self.g_ref, self.pairbuf, self.stage = at, g_ref, pairbuf, stage
        self.far, self.edge, self.send2, self.edge_sem = far, edge, send2, edge_sem
        chips = at.chips
        self.swaps, self.across = {}, {}
        for step in range(chips + 1):
            self.swaps[step] = remote(
                g_ref.at[self.slot_of(step, 1 - at.core)],
                pairbuf.at[step],
                send1.at[step],
                recv1.at[step],
                (at.band, at.partner),
            )
        for step in range(1, chips):
            self.across[step] = remote(
                stage.at[step - 1],
                far.at[step - 1],
                send2.at[step - 1],
                far_sem.at[step - 1],
                (at.band, 2 * lax.rem(at.chip + step, chips) + at.core),
            )
        self.below = (at.core == 1) & (at.band > 0)
        self.above = (at.core == 0) & (at.band < at.bands - 1)

    def slot_of(self, step, which):
        at = self.at
        if step == at.chips:
            return (1 - which) * (at.subs + 1)
        return 1 + 2 * lax.rem(at.chip + step, at.chips) + which

    def border(self, b, s, chip):
        at = self.at
        last = at.chips - 1
        return remote(
            self.stage.at[last], self.edge.at[chip], self.send2.at[last], self.edge_sem.at[chip],
            (b, s),
        )

    def swap(self, step):
        self.swaps[step].start()

    def combined(self, step):
        self.swaps[step].wait_recv()
        mine = self.g_ref[self.slot_of(step, self.at.core)]
        return mine.astype(F32) + self.pairbuf[step].astype(F32)

    def send_across(self, step):
        self.stage[step - 1] = self.combined(step).astype(BF16)
        self.across[step].start()

    def send_border(self):
        at = self.at
        self.stage[at.chips - 1] = self.combined(at.chips).astype(BF16)

        @pl.when(self.below)
        def _():
            self.border(at.band - 1, at.subs - 1, at.chip).start()

        @pl.when(self.above)
        def _():
            self.border(at.band + 1, 0, at.chip).start()

    def total(self, o_ref):
        at = self.at
        total = self.combined(0)
        for step, copy in self.across.items():
            copy.wait_recv()
            total = total + self.far[step - 1].astype(F32)
        o_ref[...] = total

        def add_edges():
            extra = o_ref[...]
            for k in range(at.chips):
                self.border(at.band, at.partner, k).wait_recv()
                extra = extra + self.edge[k].astype(F32)
            o_ref[...] = extra

        @pl.when((at.me == at.subs - 1) & (at.band < at.bands - 1))
        def _():
            add_edges()

        @pl.when((at.me == 0) & (at.band > 0))
        def _():
            add_edges()

    def finish(self):
        at = self.at
        for copy in list(self.swaps.values()) + list(self.across.values()):
            copy.wait_send()

        @pl.when(self.below)
        def _():
            self.border(at.band - 1, at.subs - 1, at.chip).wait_send()

        @pl.when(self.above)
        def _():
            self.border(at.band + 1, 0, at.chip).wait_send()


def return_scratch(chips, block):
    dma = pltpu.SemaphoreType.DMA
    return [
        pltpu.VMEM((chips + 1,) + block, BF16),
        pltpu.VMEM((chips,) + block, BF16),
        pltpu.VMEM((chips,) + block, BF16),
        pltpu.VMEM((chips,) + block, BF16),
        dma((chips + 1,)),
        dma((chips + 1,)),
        dma((chips,)),
        dma((chips,)),
        dma((chips,)),
    ]


class Reduce:
    def __init__(self, at, v, o, r1, a1, r2, r3, s1, q1, s2, q2, s3, q3, s4, q4, s5, q5):
        self.at, self.v, self.o = at, v, o
        self.r1, self.a1, self.r2, self.r3 = r1, a1, r2, r3
        device = (at.band, at.partner)
        self.mine = at.chip * INNER + at.inner
        self.pair = remote(v.at[1 - at.core], r1, s1.at[0], q1.at[0], device)
        self.spread, self.back, self.relays = [], [], []
        own = o.at[at.core, self.mine]
        self.relays.append(remote(own, own, s5.at[0], q5.at[0], device))
        for dk in range(at.chips):
            for di in range(INNER):
                n = dk * INNER + di
                if n == 0:
                    continue
                chip, inner = lax.rem(at.chip + dk, at.chips), lax.rem(at.inner + di, INNER)
                goal = (at.outer * INNER + inner, 2 * chip + at.core)
                self.spread.append(
                    remote(a1.at[chip * INNER + inner], r2.at[n - 1], s2.at[n - 1], q2.at[n - 1], goal)
                )
                self.back.append(remote(own, own, s4.at[n - 1], q4.at[n - 1], goal))
                chip = lax.rem(at.chip + at.chips - dk, at.chips)
                inner = lax.rem(at.inner + INNER - di, INNER)
                part = o.at[at.core, chip * INNER + inner]
                self.relays.append(remote(part, part, s5.at[n], q5.at[n], device))
        self.exchange = []
        for i in range(1, at.outers):
            goal = (lax.rem(at.outer + i, at.outers) * INNER + at.inner, at.me)
            self.exchange.append(
                remote(r3.at[at.outer], r3.at[at.outer], s3.at[i - 1], q3.at[i - 1], goal)
            )

    def start(self):
        self.pair.start()

    def to_quarters(self):
        self.pair.wait_recv()
        self.a1[...] = (self.v[self.at.core].astype(F32) + self.r1[...].astype(F32)).astype(BF16)
        for copy in self.spread:
            copy.start()

    def to_exchange(self):
        total = self.a1[self.mine].astype(F32)
        for n, copy in enumerate(self.spread):
            copy.wait_recv()
            total = total + self.r2[n].astype(F32)
        self.r3[self.at.outer] = total.astype(BF16)
        for copy in self.exchange:
            copy.start()

    def to_back(self):
        for copy in self.exchange:
            copy.wait_recv()
        total = self.r3[0].astype(F32)
        for i in range(1, self.at.outers):
            total = total + self.r3[i].astype(F32)
        self.o[self.at.core, self.mine] = total.astype(BF16)
        for copy in self.back:
            copy.start()
        self.relays[0].start()

    def to_relay(self):
        for copy, relay in zip(self.back, self.relays[1:]):
            copy.wait_recv()
            relay.start()

    def finish(self):
        for copy in self.relays:
            copy.wait_recv()
        for copy in [self.pair] + self.spread + self.exchange + self.back + self.relays:
            copy.wait_send()


def reduce_shape(chips, rows, cols):
    quarters = chips * INNER
    return (2, quarters, rows // (2 * quarters), cols)


def reduce_scratch(chips, outers, rows, cols):
    dma = pltpu.SemaphoreType.DMA
    shape = reduce_shape(chips, rows, cols)
    quarters, piece = shape[1], shape[2:]
    return [
        pltpu.VMEM(shape[1:], BF16),
        pltpu.VMEM(shape[1:], BF16),
        pltpu.VMEM((quarters - 1,) + piece, BF16),
        pltpu.VMEM((outers,) + piece, BF16),
        dma((1,)),
        dma((1,)),
        dma((quarters - 1,)),
        dma((quarters - 1,)),
        dma((outers - 1,)),
        dma((outers - 1,)),
        dma((quarters - 1,)),
        dma((quarters - 1,)),
        dma((quarters,)),
        dma((quarters,)),
    ]


def take(refs, count):
    return refs[:count], refs[count:]


def whole_kernel(
    bands, subs, sizes,
    x_in, mesh_ref, we_in, ws_in, wd_in, wedge_in, wp_in, wr_in, gs_ref, gi_ref, mi_ref, cot_ref,
    mesh_out, grid_out, src_full, edge_full,
    xw, we, ws, wd, wedge, wp, wr, proj, rows_even, rows_odd, hid_t, slope_pre, dest,
    act, slope, normed, inverse, out_tile, encoded, hidden_mesh, receiver, picks,
    qwindow, mslope, rgrad, qslots, qgrad, mgrad, ugrad, grad, bgrad, edge_v,
    wgrad, left_v, right_v, gslots, src_out, edge_out, gv_ref, mv_ref, local,
    *rest,
):
    nodes, rows, enc, fan, latent, tile = sizes
    slots = subs + 2
    cols = latent // LANES
    half = latent // 2
    gathered = (rows_even, rows_odd)
    at = Place(bands, subs)
    fetch_x, rest = take(rest, 2)
    fetch_q, rest = take(rest, 2)
    return_q, rest = take(rest, 9)
    return_g, rest = take(rest, 9)
    scratch_e, rest = take(rest, 14)
    scratch_l, rest = take(rest, 14)
    scratch_r, rest = take(rest, 14)

    def load(src, dst, index):
        copy = pltpu.make_async_copy(src, dst, local.at[index])
        copy.start()
        return copy

    entry_barrier(at)
    xfetch = Fetch(at, x_in, xw, *fetch_x)
    xfetch.start()
    own_x = load(x_in, xw.at[1 + at.me], 0)
    loads = [
        load(src, dst, 1 + i)
        for i, (src, dst) in enumerate(
            [(we_in, we), (ws_in, ws), (wd_in, wd), (wedge_in, wedge), (wp_in, wp), (wr_in, wr)]
        )
    ]
    xfetch.clear()
    for k in range(enc):
        gv_ref[0:1, k * rows : (k + 1) * rows] = gi_ref[k : k + 1, :]
    for j in range(fan):
        mv_ref[0:1, j * rows : (j + 1) * rows] = mi_ref[j : j + 1, :]

    def embed(slot):
        for part in range(2):
            n = nodes // 2
            pre = contract(xw[slot, :, part * n : (part + 1) * n], we[...], 0, 0)
            active, slope_value = silu_pair(pre)
            active = active.astype(BF16)
            slope_pre[slot, part * n : (part + 1) * n] = slope_value.astype(BF16)
            column = pl.multiple_of(slot * nodes + part * n, n)
            hid_t[:, pl.ds(column, n)] = active.T
            value = jnp.dot(active, ws[...], preferred_element_type=F32)
            for j in range(cols):
                start = (slot * nodes + part * n) * cols + j
                proj[pl.ds(start, n, stride=cols), :] = value[:, j * LANES : (j + 1) * LANES]

    def step(i, carry):
        @pl.when(i == 1)
        def _():
            xfetch.wait_partner()

        for k in range(1, at.chips):
            @pl.when(i == 2 * k)
            def _(k=k):
                xfetch.wait_near(k)

            @pl.when(i == 2 * k + 1)
            def _(k=k):
                xfetch.wait_far(k)

        @pl.when(i == subs)
        def _():
            xfetch.wait_border()

        @pl.when(i == subs + 1)
        def _():
            xfetch.wait_other_border()

        odd = lax.rem(i, 2)
        side = at.core + odd - 2 * at.core * odd
        inside = 1 + 2 * lax.rem(at.chip + at.chips - i // 2 + at.chips, at.chips) + side
        outside = (1 - side) * (subs + 1)
        embed(jnp.where(i < subs, inside, outside))
        return carry

    for copy in loads[:3]:
        copy.wait()
    own_x.wait()
    dest[...] = jnp.dot(mesh_ref[...], wd[...], preferred_element_type=F32)
    lax.fori_loop(0, slots, step, 0)
    for copy in loads[3:]:
        copy.wait()

    chunk = tile * rows
    chunks = enc // tile
    first = at.band * (nodes * subs) - nodes
    encoded[...] = jnp.zeros_like(encoded)

    def gather(c, low, high):
        for r in range(low, high):
            k, m = divmod(c * chunk + r, rows)
            index = jnp.maximum(gs_ref[k, m] - first, 0) * cols
            gathered[c % 2][r * cols : (r + 1) * cols, :] = proj[pl.ds(index, cols), :]

    def before(c, t):
        base = (c * tile + t) * rows
        for j in range(cols):
            lane = slice(j * LANES, (j + 1) * LANES)
            value = gathered[c % 2][pl.ds(t * rows * cols + j, rows, stride=cols), :]
            active, slope_value = silu_pair(value + dest[:, lane])
            act[base : base + rows, lane] = active.astype(BF16)
            slope[base : base + rows, lane] = slope_value.astype(BF16)

    def norm(c, t):
        base = (c * tile + t) * rows
        out = out_tile[t * rows : (t + 1) * rows, :]
        out = out - jnp.mean(out, axis=-1, keepdims=True)
        factor = lax.rsqrt(jnp.mean(out * out, axis=-1, keepdims=True) + EPSILON)
        out = out * factor
        inverse[base : base + rows, :] = jnp.broadcast_to(factor, (rows, LANES))
        normed[base : base + rows, :] = out.astype(BF16)
        encoded[...] += out

    gather(0, 0, chunk)
    share = rows // 2
    for c in range(chunks):
        more = c + 1 < chunks
        for t in range(tile):
            if more:
                gather(c + 1, t * share, (t + 1) * share)
            before(c, t)
        out_tile[...] = jnp.dot(
            act[c * chunk : (c + 1) * chunk, :], wedge[...], preferred_element_type=F32
        )
        for t in range(tile):
            if more:
                gather(c + 1, (tile + t) * share, (tile + t + 1) * share)
            norm(c, t)

    mesh = mesh_ref[...].astype(F32) + encoded[...] * (1.0 / math.sqrt(enc))
    hidden_mesh[...] = mesh.astype(BF16)
    qwindow[1 + at.me] = jnp.dot(hidden_mesh[...], wp[...], preferred_element_type=F32).astype(BF16)
    qfetch = Fetch(at, qwindow.at[1 + at.me], qwindow, *fetch_q)
    qfetch.start()
    qfetch.clear()
    receiver[...] = jnp.dot(hidden_mesh[...], wr[...], preferred_element_type=F32)
    count = slots * rows
    mesh_first = at.band * (rows * subs) - rows
    node = lax.broadcasted_iota(jnp.int32, (count, fan * rows), 0)
    picks[...] = jnp.where(node == mv_ref[...] - mesh_first, 1.0, 0.0).astype(BF16)
    qfetch.wait_partner()
    for k in range(1, at.chips):
        qfetch.wait_near(k)
    qfetch.wait_border()
    for k in range(1, at.chips):
        qfetch.wait_far(k)
    qfetch.wait_other_border()
    mesh_before = contract(picks[...], qwindow[...].reshape(count, latent), 0, 0)
    upstream = cot_ref[...].astype(F32)
    scaled = upstream * (1.0 / math.sqrt(fan))
    summed = jnp.zeros((rows, latent), F32)
    received = jnp.zeros((rows, latent), F32)
    for j in range(fan):
        value = mesh_before[j * rows : (j + 1) * rows] + receiver[...]
        active, slope_value = silu_pair(value)
        summed = summed + active
        slope_value = scaled * slope_value
        received = received + slope_value
        mslope[j * rows : (j + 1) * rows] = slope_value.astype(BF16)
    window = jnp.dot(picks[...], mslope[...], preferred_element_type=F32)
    qslots[...] = window.astype(BF16).reshape(slots, rows, latent)
    qreturn = Return(at, qslots, *return_q)
    for s in list(range(1, at.chips)) + [at.chips, 0]:
        qreturn.swap(s)
    mesh_out[...] = (hidden_mesh[...].astype(F32) + summed * (1.0 / math.sqrt(fan))).astype(BF16)
    rgrad[...] = received.astype(BF16)
    for s in range(1, at.chips):
        qreturn.send_across(s)
    qreturn.send_border()
    mgrad[...] = upstream + contract(rgrad[...], wr[...], 1, 1)
    qreturn.total(qgrad)
    upper = mgrad[...] + contract(qgrad[...].astype(BF16), wp[...], 1, 1)
    upper = upper * (1.0 / math.sqrt(enc))
    mgrad[...] = upper
    ugrad[...] = upper - jnp.mean(upper, axis=-1, keepdims=True)

    def decode(k, carry):
        base = pl.multiple_of(k * rows, rows)
        value = normed[pl.ds(base, rows), :].astype(F32)
        both = jnp.mean(mgrad[...] * value, axis=-1, keepdims=True)
        out = (ugrad[...] - value * both) * inverse[pl.ds(base, rows), 0:1]
        grad[pl.ds(base, rows), :] = out.astype(BF16)
        return carry

    lax.fori_loop(0, enc, decode, 0, unroll=8)
    edge_value = contract(act[...], grad[...], 0, 0).astype(BF16)
    edge_v[...] = edge_value.reshape(edge_v.shape)
    edge = Reduce(at, edge_v, edge_out, *scratch_e)
    left = Reduce(at, left_v, src_out.at[:, :, :, 0:half], *scratch_l)
    right = Reduce(at, right_v, src_out.at[:, :, :, half:latent], *scratch_r)
    edge.start()
    back = contract(grad[...], wedge[...], 1, 1) * slope[...].astype(F32)
    bgrad[...] = back.astype(BF16)

    def scatter(h, slot):
        lane = slice(h * half, (h + 1) * half)
        node = lax.broadcasted_iota(jnp.int32, (nodes, enc * rows), 0) + (first + slot * nodes)
        hot = jnp.where(node == gv_ref[...], 1.0, 0.0).astype(BF16)
        total = jnp.dot(hot, bgrad[:, lane], preferred_element_type=F32)
        wgrad[pl.ds(pl.multiple_of(slot * nodes, nodes), nodes), lane] = total.astype(BF16)

    def source(h, ref):
        lane = slice(h * half, (h + 1) * half)
        total = jnp.dot(hid_t[...], wgrad[:, lane], preferred_element_type=F32)
        ref[...] = total.astype(BF16).reshape(ref.shape)

    def grid_back(slot):
        value = contract(wgrad[pl.ds(pl.multiple_of(slot * nodes, nodes), nodes), :], ws[...], 1, 1)
        value = (value * slope_pre[slot].astype(F32)).astype(BF16)
        gslots[slot] = contract(we[...], value, 1, 1).astype(BF16)

    greturn = Return(at, gslots, *return_g)

    def pair(s, work):
        def one(which, carry):
            if s == at.chips:
                slot = which * (subs + 1)
            else:
                slot = 1 + 2 * lax.rem(at.chip + s, at.chips) + which
            work(slot)
            return carry

        lax.fori_loop(0, 2, one, 0)

    def scatter_left(slot, carry):
        scatter(0, slot)
        return carry

    def scatter_right(slot):
        scatter(1, slot)

    edge.to_quarters()
    lax.fori_loop(0, slots, scatter_left, 0)
    edge.to_exchange()
    source(0, left_v)
    left.start()
    pair(at.chips, scatter_right)
    left.to_quarters()
    pair(at.chips, grid_back)
    greturn.swap(at.chips)
    for s in range(1, at.chips):
        pair(s, scatter_right)
    greturn.send_border()
    pair(0, scatter_right)
    left.to_exchange()
    source(1, right_v)
    right.start()
    for s in range(1, at.chips):
        pair(s, grid_back)
        greturn.swap(s)
    right.to_quarters()
    for s in range(1, at.chips):
        greturn.send_across(s)
    pair(0, grid_back)
    greturn.swap(0)
    right.to_exchange()
    edge.to_back()
    left.to_back()
    greturn.total(grid_out)
    right.to_back()
    edge.to_relay()
    left.to_relay()
    right.to_relay()
    for stream in (greturn, qreturn, xfetch, qfetch, edge, left):
        stream.finish()
    edge_full[...] = edge_out[...].astype(F32).reshape(latent, latent)
    src_full[:, 0:half] = src_out[:, :, :, 0:half].astype(F32).reshape(latent, half)
    right.finish()
    src_full[:, half:latent] = src_out[:, :, :, half:latent].astype(F32).reshape(latent, half)


def whole(bands, subs, sizes, channels, args):
    nodes, rows, enc, fan, latent, tile = sizes
    chips, outers, slots = subs // 2, bands // INNER, subs + 2
    edges = rows * enc
    half = latent // 2
    dma = pltpu.SemaphoreType.DMA
    square = pltpu.VMEM((latent, latent), BF16)
    small = pltpu.VMEM((rows, latent), F32)
    small_low = pltpu.VMEM((rows, latent), BF16)
    wide = pltpu.VMEM((edges, latent), BF16)
    scratch = [
        pltpu.VMEM((slots, channels, nodes), BF16),
        pltpu.VMEM((channels, latent), BF16),
        square, square, square, square, square,
        pltpu.VMEM((slots * nodes * latent // LANES, LANES), F32),
        pltpu.VMEM((tile * rows * latent // LANES, LANES), F32),
        pltpu.VMEM((tile * rows * latent // LANES, LANES), F32),
        pltpu.VMEM((latent, slots * nodes), BF16),
        pltpu.VMEM((slots, nodes, latent), BF16),
        small,
        wide, wide, wide,
        pltpu.VMEM((edges, LANES), F32),
        pltpu.VMEM((tile * rows, latent), F32),
        small, small_low, small,
        pltpu.VMEM((slots * rows, fan * rows), BF16),
        pltpu.VMEM((slots, rows, latent), BF16),
        pltpu.VMEM((fan * rows, latent), BF16),
        small_low,
        pltpu.VMEM((slots, rows, latent), BF16),
        small, small, small,
        wide, wide,
        pltpu.VMEM(reduce_shape(chips, latent, latent), BF16),
        pltpu.VMEM((slots * nodes, latent), BF16),
        pltpu.VMEM(reduce_shape(chips, latent, half), BF16),
        pltpu.VMEM(reduce_shape(chips, latent, half), BF16),
        pltpu.VMEM((slots, channels, nodes), BF16),
        pltpu.VMEM(reduce_shape(chips, latent, latent), BF16),
        pltpu.VMEM(reduce_shape(chips, latent, latent), BF16),
        pltpu.VMEM((1, edges), jnp.int32),
        pltpu.VMEM((1, fan * rows), jnp.int32),
        dma((7,)),
    ]
    scratch += fetch_scratch(chips, subs) * 2
    scratch += return_scratch(chips, (rows, latent)) + return_scratch(chips, (channels, nodes))
    scratch += reduce_scratch(chips, outers, latent, latent)
    scratch += reduce_scratch(chips, outers, latent, half) * 2
    return pl.pallas_call(
        functools.partial(whole_kernel, bands, subs, sizes),
        out_shape=[
            pltpu.VMEM((rows, latent), BF16),
            pltpu.VMEM((channels, nodes), F32),
            pltpu.VMEM((latent, latent), F32),
            pltpu.VMEM((latent, latent), F32),
        ],
        in_specs=[ANY, VMEM] + [ANY] * 6 + [SMEM, VMEM, VMEM, VMEM],
        out_specs=[VMEM] * 4,
        scratch_shapes=scratch,
        compiler_params=pltpu.CompilerParams(collective_id=0, has_side_effects=True, vmem_limit_bytes=60 << 20),
        name="whole",
    )(*args)


def finish_kernel(count, *refs):
    ins, outs, sems = refs[:count], refs[count : 2 * count], refs[2 * count]
    copies = [pltpu.make_async_copy(ins[i], outs[i], sems.at[i]) for i in range(count)]
    for copy in copies:
        copy.start()
    for copy in copies:
        copy.wait()


def finish(arrays):
    count = len(arrays)
    return pl.pallas_call(
        functools.partial(finish_kernel, count),
        out_shape=[jax.ShapeDtypeStruct(array.shape, array.dtype) for array in arrays],
        in_specs=[VMEM] * count,
        out_specs=[ANY] * count,
        scratch_shapes=[pltpu.SemaphoreType.DMA((count,))],
        compiler_params=pltpu.CompilerParams(vmem_limit_bytes=1 << 20),
        name="finish",
    )(*arrays)


def body(
    bands, subs,
    grid_x, mesh_in, w_embed, w_src, w_dst, w_edge, w_proc, w_recv, g2m_src, mesh_src, cotangent
):
    latent = w_src.shape[0]
    channels, nodes = grid_x.shape
    rows, enc = g2m_src.shape
    fan = mesh_src.shape[1]
    sizes = (nodes, rows, enc, fan, latent, 4)
    by_edge = g2m_src.T
    args = (
        grid_x, mesh_in, w_embed, w_src, w_dst, w_edge, w_proc, w_recv,
        by_edge, by_edge, mesh_src.T, cotangent,
    )
    return finish(whole(bands, subs, sizes, channels, args))


def solution(mesh):
    nodes = P(("band", "sub"), None)
    placed = (P(None, ("band", "sub")), nodes) + (P(),) * 6 + (nodes,) * 3
    return jax.shard_map(
        functools.partial(body, mesh.shape["band"], mesh.shape["sub"]),
        mesh=mesh,
        in_specs=placed,
        out_specs=(nodes, P(None, ("band", "sub")), P(), P()),
        check_vma=False,
    )
```

```python
import functools
import math

import jax
import jax.numpy as jnp
from jax import lax
from jax.experimental import pallas as pl
from jax.experimental.pallas import tpu as pltpu
from jax.sharding import PartitionSpec as P

EPSILON = 1e-05
F32 = jnp.float32
BF16 = jnp.bfloat16
LANES = 128
INNER = 2
VMEM = pl.BlockSpec(memory_space=pltpu.VMEM)
SMEM = pl.BlockSpec(memory_space=pltpu.SMEM)
ANY = pl.BlockSpec(memory_space=pl.ANY)


def contract(left, right, left_dim, right_dim):
    return lax.dot_general(
        left, right, (((left_dim,), (right_dim,)), ((), ())), preferred_element_type=F32
    )


def silu_pair(value):
    sigma = 0.5 * jnp.tanh(0.5 * value) + 0.5
    active = value * sigma
    return active, sigma + active * (1.0 - sigma)


def remote(src, dst, send, recv, device):
    return pltpu.make_async_remote_copy(
        src_ref=src,
        dst_ref=dst,
        send_sem=send,
        recv_sem=recv,
        device_id=device,
        device_id_type=pl.DeviceIdType.MESH,
    )


def greet(barrier, device):
    pl.semaphore_signal(barrier, inc=1, device_id=device, device_id_type=pl.DeviceIdType.MESH)


class Place:
    def __init__(self, bands, subs):
        self.bands, self.subs = bands, subs
        self.band, self.me = lax.axis_index("band"), lax.axis_index("sub")
        self.core = lax.rem(self.me, 2)
        self.chip = self.me // 2
        self.partner = self.me + 1 - 2 * self.core
        self.chips = subs // 2
        self.outer, self.inner = self.band // INNER, lax.rem(self.band, INNER)
        self.outers = bands // INNER


def entry_barrier(at):
    barrier = pltpu.get_barrier_semaphore()
    for step in range(1, at.subs):
        greet(barrier, (at.band, lax.rem(at.me + step, at.subs)))

    @pl.when(at.band > 0)
    def _():
        for other in range(at.subs):
            greet(barrier, (at.band - 1, other))

    @pl.when(at.band < at.bands - 1)
    def _():
        for other in range(at.subs):
            greet(barrier, (at.band + 1, other))

    for i in range(1, at.outers):
        greet(barrier, (lax.rem(at.outer + i, at.outers) * INNER + at.inner, at.me))
    sides = jnp.minimum(at.band, 1) + jnp.minimum(at.bands - 1 - at.band, 1)
    pl.semaphore_wait(barrier, at.subs - 1 + at.subs * sides + at.outers - 1)


class Fetch:
    def __init__(self, at, src, o_ref, send, recv):
        self.at, self.src, self.o_ref, self.send, self.recv = at, src, o_ref, send, recv
        chips = at.chips
        self.across = [
            self.push(src, 1 + at.me, at.band, 2 * lax.rem(at.chip + k, chips) + at.core, k - 1)
            for k in range(1, chips)
        ]
        self.pair = self.push(src, 1 + at.me, at.band, at.partner, chips - 1)
        self.rising = (at.me == at.subs - 1) & (at.band < at.bands - 1)
        self.falling = (at.me == 0) & (at.band > 0)
        self.direct_below = (at.core == 1) & (at.band > 0)
        self.direct_above = (at.core == 0) & (at.band < at.bands - 1)
        top = at.subs + 1
        self.relay_below = self.push(o_ref.at[0], 0, at.band, at.partner, 4 * chips - 1)
        self.relay_above = self.push(o_ref.at[top], top, at.band, at.partner, 4 * chips)
        self.relays = []
        for k in range(1, chips):
            slot = self.near(k)
            self.relays.append(
                self.push(o_ref.at[slot], slot, at.band, at.partner, 3 * chips + k - 1)
            )

    def push(self, src, slot, b, s, index):
        return remote(src, self.o_ref.at[slot], self.send.at[index], self.recv.at[slot], (b, s))

    def near(self, k):
        at = self.at
        return 1 + 2 * lax.rem(at.chip + at.chips - k, at.chips) + at.core

    def up(self, k):
        at = self.at
        return self.push(self.src, 0, at.band + 1, 2 * k + 1, at.chips + k)

    def down(self, k):
        at = self.at
        return self.push(self.src, at.subs + 1, at.band - 1, 2 * k, 2 * at.chips + k)

    def arrived(self, slot):
        self.push(self.src, slot, self.at.band, self.at.partner, 0).wait_recv()

    def start(self):
        for copy in self.across:
            copy.start()
        self.pair.start()

        @pl.when(self.rising)
        def _():
            for k in range(self.at.chips):
                self.up(k).start()

        @pl.when(self.falling)
        def _():
            for k in range(self.at.chips):
                self.down(k).start()

    def clear(self):
        at = self.at
        block, kind = self.o_ref.shape[1:], self.o_ref.dtype

        @pl.when(at.band == 0)
        def _():
            self.o_ref[0] = jnp.zeros(block, kind)

        @pl.when(at.band == at.bands - 1)
        def _():
            self.o_ref[at.subs + 1] = jnp.zeros(block, kind)

    def wait_partner(self):
        self.arrived(1 + self.at.partner)

    def wait_near(self, k):
        self.arrived(self.near(k))
        self.relays[k - 1].start()

    def wait_far(self, k):
        self.arrived(self.near(k) + 1 - 2 * self.at.core)

    def wait_border(self):
        @pl.when(self.direct_below)
        def _():
            self.arrived(0)
            self.relay_below.start()

        @pl.when(self.direct_above)
        def _():
            self.arrived(self.at.subs + 1)
            self.relay_above.start()

    def wait_other_border(self):
        at = self.at

        @pl.when((at.core == 0) & (at.band > 0))
        def _():
            self.arrived(0)

        @pl.when((at.core == 1) & (at.band < at.bands - 1))
        def _():
            self.arrived(at.subs + 1)

    def finish(self):
        for copy in self.across + [self.pair] + self.relays:
            copy.wait_send()

        @pl.when(self.rising)
        def _():
            for k in range(self.at.chips):
                self.up(k).wait_send()

        @pl.when(self.falling)
        def _():
            for k in range(self.at.chips):
                self.down(k).wait_send()

        @pl.when(self.direct_below)
        def _():
            self.relay_below.wait_send()

        @pl.when(self.direct_above)
        def _():
            self.relay_above.wait_send()


def fetch_scratch(at_chips, subs):
    dma = pltpu.SemaphoreType.DMA
    return [dma((4 * at_chips + 1,)), dma((subs + 2,))]


class Return:
    def __init__(self, at, g_ref, pairbuf, stage, far, edge, send1, recv1, send2, far_sem, edge_sem):
        self.at, self.g_ref, self.pairbuf, self.stage = at, g_ref, pairbuf, stage
        self.far, self.edge, self.send2, self.edge_sem = far, edge, send2, edge_sem
        chips = at.chips
        self.swaps, self.across = {}, {}
        for step in range(chips + 1):
            self.swaps[step] = remote(
                g_ref.at[self.slot_of(step, 1 - at.core)],
                pairbuf.at[step],
                send1.at[step],
                recv1.at[step],
                (at.band, at.partner),
            )
        for step in range(1, chips):
            self.across[step] = remote(
                stage.at[step - 1],
                far.at[step - 1],
                send2.at[step - 1],
                far_sem.at[step - 1],
                (at.band, 2 * lax.rem(at.chip + step, chips) + at.core),
            )
        self.below = (at.core == 1) & (at.band > 0)
        self.above = (at.core == 0) & (at.band < at.bands - 1)

    def slot_of(self, step, which):
        at = self.at
        if step == at.chips:
            return (1 - which) * (at.subs + 1)
        return 1 + 2 * lax.rem(at.chip + step, at.chips) + which

    def border(self, b, s, chip):
        at = self.at
        last = at.chips - 1
        return remote(
            self.stage.at[last], self.edge.at[chip], self.send2.at[last], self.edge_sem.at[chip],
            (b, s),
        )

    def swap(self, step):
        self.swaps[step].start()

    def combined(self, step):
        self.swaps[step].wait_recv()
        mine = self.g_ref[self.slot_of(step, self.at.core)]
        return mine.astype(F32) + self.pairbuf[step].astype(F32)

    def send_across(self, step):
        self.stage[step - 1] = self.combined(step).astype(BF16)
        self.across[step].start()

    def send_border(self):
        at = self.at
        self.stage[at.chips - 1] = self.combined(at.chips).astype(BF16)

        @pl.when(self.below)
        def _():
            self.border(at.band - 1, at.subs - 1, at.chip).start()

        @pl.when(self.above)
        def _():
            self.border(at.band + 1, 0, at.chip).start()

    def total(self, o_ref):
        at = self.at
        total = self.combined(0)
        for step, copy in self.across.items():
            copy.wait_recv()
            total = total + self.far[step - 1].astype(F32)
        o_ref[...] = total

        def add_edges():
            extra = o_ref[...]
            for k in range(at.chips):
                self.border(at.band, at.partner, k).wait_recv()
                extra = extra + self.edge[k].astype(F32)
            o_ref[...] = extra

        @pl.when((at.me == at.subs - 1) & (at.band < at.bands - 1))
        def _():
            add_edges()

        @pl.when((at.me == 0) & (at.band > 0))
        def _():
            add_edges()

    def finish(self):
        at = self.at
        for copy in list(self.swaps.values()) + list(self.across.values()):
            copy.wait_send()

        @pl.when(self.below)
        def _():
            self.border(at.band - 1, at.subs - 1, at.chip).wait_send()

        @pl.when(self.above)
        def _():
            self.border(at.band + 1, 0, at.chip).wait_send()


def return_scratch(chips, block):
    dma = pltpu.SemaphoreType.DMA
    return [
        pltpu.VMEM((chips + 1,) + block, BF16),
        pltpu.VMEM((chips,) + block, BF16),
        pltpu.VMEM((chips,) + block, BF16),
        pltpu.VMEM((chips,) + block, BF16),
        dma((chips + 1,)),
        dma((chips + 1,)),
        dma((chips,)),
        dma((chips,)),
        dma((chips,)),
    ]


class Reduce:
    def __init__(self, at, v, o, r1, a1, r2, r3, s1, q1, s2, q2, s3, q3, s4, q4, s5, q5):
        self.at, self.v, self.o = at, v, o
        self.r1, self.a1, self.r2, self.r3 = r1, a1, r2, r3
        device = (at.band, at.partner)
        self.mine = at.chip * INNER + at.inner
        self.pair = remote(v.at[1 - at.core], r1, s1.at[0], q1.at[0], device)
        self.spread, self.back, self.relays = [], [], []
        own = o.at[at.core, self.mine]
        self.relays.append(remote(own, own, s5.at[0], q5.at[0], device))
        for dk in range(at.chips):
            for di in range(INNER):
                n = dk * INNER + di
                if n == 0:
                    continue
                chip, inner = lax.rem(at.chip + dk, at.chips), lax.rem(at.inner + di, INNER)
                goal = (at.outer * INNER + inner, 2 * chip + at.core)
                self.spread.append(
                    remote(a1.at[chip * INNER + inner], r2.at[n - 1], s2.at[n - 1], q2.at[n - 1], goal)
                )
                self.back.append(remote(own, own, s4.at[n - 1], q4.at[n - 1], goal))
                chip = lax.rem(at.chip + at.chips - dk, at.chips)
                inner = lax.rem(at.inner + INNER - di, INNER)
                part = o.at[at.core, chip * INNER + inner]
                self.relays.append(remote(part, part, s5.at[n], q5.at[n], device))
        self.exchange = []
        for i in range(1, at.outers):
            goal = (lax.rem(at.outer + i, at.outers) * INNER + at.inner, at.me)
            self.exchange.append(
                remote(r3.at[at.outer], r3.at[at.outer], s3.at[i - 1], q3.at[i - 1], goal)
            )

    def start(self):
        self.pair.start()

    def to_quarters(self):
        self.pair.wait_recv()
        self.a1[...] = (self.v[self.at.core].astype(F32) + self.r1[...].astype(F32)).astype(BF16)
        for copy in self.spread:
            copy.start()

    def to_exchange(self):
        total = self.a1[self.mine].astype(F32)
        for n, copy in enumerate(self.spread):
            copy.wait_recv()
            total = total + self.r2[n].astype(F32)
        self.r3[self.at.outer] = total.astype(BF16)
        for copy in self.exchange:
            copy.start()

    def to_back(self):
        for copy in self.exchange:
            copy.wait_recv()
        total = self.r3[0].astype(F32)
        for i in range(1, self.at.outers):
            total = total + self.r3[i].astype(F32)
        self.o[self.at.core, self.mine] = total.astype(BF16)
        for copy in self.back:
            copy.start()
        self.relays[0].start()

    def to_relay(self):
        for copy, relay in zip(self.back, self.relays[1:]):
            copy.wait_recv()
            relay.start()

    def finish(self):
        for copy in self.relays:
            copy.wait_recv()
        for copy in [self.pair] + self.spread + self.exchange + self.back + self.relays:
            copy.wait_send()


def reduce_shape(chips, rows, cols):
    quarters = chips * INNER
    return (2, quarters, rows // (2 * quarters), cols)


def reduce_scratch(chips, outers, rows, cols):
    dma = pltpu.SemaphoreType.DMA
    shape = reduce_shape(chips, rows, cols)
    quarters, piece = shape[1], shape[2:]
    return [
        pltpu.VMEM(shape[1:], BF16),
        pltpu.VMEM(shape[1:], BF16),
        pltpu.VMEM((quarters - 1,) + piece, BF16),
        pltpu.VMEM((outers,) + piece, BF16),
        dma((1,)),
        dma((1,)),
        dma((quarters - 1,)),
        dma((quarters - 1,)),
        dma((outers - 1,)),
        dma((outers - 1,)),
        dma((quarters - 1,)),
        dma((quarters - 1,)),
        dma((quarters,)),
        dma((quarters,)),
    ]


def take(refs, count):
    return refs[:count], refs[count:]


def whole_kernel(
    bands, subs, sizes,
    x_in, mesh_ref, we_in, ws_in, wd_in, wedge_in, wp_in, wr_in, gs_ref, gi_ref, mi_ref, cot_ref,
    mesh_out, grid_out, src_full, edge_full,
    xw, we, ws, wd, wedge, wp, wr, proj, rows_even, rows_odd, hid_t, slope_pre, dest,
    act, slope, normed, inverse, out_tile, encoded, hidden_mesh, receiver, picks,
    qwindow, mslope, rgrad, qslots, qgrad, mgrad, ugrad, grad, bgrad, edge_v,
    wgrad, left_v, right_v, gslots, src_out, edge_out, gv_ref, mv_ref, local,
    *rest,
):
    nodes, rows, enc, fan, latent, tile = sizes
    slots = subs + 2
    cols = latent // LANES
    half = latent // 2
    gathered = (rows_even, rows_odd)
    at = Place(bands, subs)
    fetch_x, rest = take(rest, 2)
    fetch_q, rest = take(rest, 2)
    return_q, rest = take(rest, 9)
    return_g, rest = take(rest, 9)
    scratch_e, rest = take(rest, 14)
    scratch_l, rest = take(rest, 14)
    scratch_r, rest = take(rest, 14)

    def load(src, dst, index):
        copy = pltpu.make_async_copy(src, dst, local.at[index])
        copy.start()
        return copy

    entry_barrier(at)
    xfetch = Fetch(at, x_in, xw, *fetch_x)
    xfetch.start()
    own_x = load(x_in, xw.at[1 + at.me], 0)
    loads = [
        load(src, dst, 1 + i)
        for i, (src, dst) in enumerate(
            [(we_in, we), (ws_in, ws), (wd_in, wd), (wedge_in, wedge), (wp_in, wp), (wr_in, wr)]
        )
    ]
    xfetch.clear()
    for k in range(enc):
        gv_ref[0:1, k * rows : (k + 1) * rows] = gi_ref[k : k + 1, :]
    for j in range(fan):
        mv_ref[0:1, j * rows : (j + 1) * rows] = mi_ref[j : j + 1, :]

    def embed(slot):
        for part in range(2):
            n = nodes // 2
            pre = contract(xw[slot, :, part * n : (part + 1) * n], we[...], 0, 0)
            active, slope_value = silu_pair(pre)
            active = active.astype(BF16)
            slope_pre[slot, part * n : (part + 1) * n] = slope_value.astype(BF16)
            column = pl.multiple_of(slot * nodes + part * n, n)
            hid_t[:, pl.ds(column, n)] = active.T
            value = jnp.dot(active, ws[...], preferred_element_type=F32)
            for j in range(cols):
                start = (slot * nodes + part * n) * cols + j
                proj[pl.ds(start, n, stride=cols), :] = value[:, j * LANES : (j + 1) * LANES]

    def step(turn, carry):
        i = jnp.where(turn == subs - 1, subs, jnp.where(turn == subs, subs - 1, turn))

        @pl.when(i == 1)
        def _():
            xfetch.wait_partner()

        for k in range(1, at.chips):
            @pl.when(i == 2 * k)
            def _(k=k):
                xfetch.wait_near(k)

            @pl.when(i == 2 * k + 1)
            def _(k=k):
                xfetch.wait_far(k)

        @pl.when(i == subs)
        def _():
            xfetch.wait_border()

        @pl.when(i == subs + 1)
        def _():
            xfetch.wait_other_border()

        odd = lax.rem(i, 2)
        side = at.core + odd - 2 * at.core * odd
        inside = 1 + 2 * lax.rem(at.chip + at.chips - i // 2 + at.chips, at.chips) + side
        outside = (1 - side) * (subs + 1)
        embed(jnp.where(i < subs, inside, outside))
        return carry

    for copy in loads[:3]:
        copy.wait()
    own_x.wait()
    dest[...] = jnp.dot(mesh_ref[...], wd[...], preferred_element_type=F32)
    lax.fori_loop(0, slots, step, 0)
    for copy in loads[3:]:
        copy.wait()

    chunk = tile * rows
    chunks = enc // tile
    first = at.band * (nodes * subs) - nodes
    encoded[...] = jnp.zeros_like(encoded)

    def gather(c, low, high):
        for r in range(low, high):
            k, m = divmod(c * chunk + r, rows)
            index = jnp.maximum(gs_ref[k, m] - first, 0) * cols
            gathered[c % 2][r * cols : (r + 1) * cols, :] = proj[pl.ds(index, cols), :]

    def before(c, t):
        base = (c * tile + t) * rows
        for j in range(cols):
            lane = slice(j * LANES, (j + 1) * LANES)
            value = gathered[c % 2][pl.ds(t * rows * cols + j, rows, stride=cols), :]
            active, slope_value = silu_pair(value + dest[:, lane])
            act[base : base + rows, lane] = active.astype(BF16)
            slope[base : base + rows, lane] = slope_value.astype(BF16)

    def norm(c, t):
        base = (c * tile + t) * rows
        out = out_tile[t * rows : (t + 1) * rows, :]
        out = out - jnp.mean(out, axis=-1, keepdims=True)
        factor = lax.rsqrt(jnp.mean(out * out, axis=-1, keepdims=True) + EPSILON)
        out = out * factor
        inverse[base : base + rows, :] = jnp.broadcast_to(factor, (rows, LANES))
        normed[base : base + rows, :] = out.astype(BF16)
        encoded[...] += out

    gather(0, 0, chunk)
    share = rows // 2
    for c in range(chunks):
        more = c + 1 < chunks
        for t in range(tile):
            if more:
                gather(c + 1, t * share, (t + 1) * share)
            before(c, t)
        out_tile[...] = jnp.dot(
            act[c * chunk : (c + 1) * chunk, :], wedge[...], preferred_element_type=F32
        )
        for t in range(tile):
            if more:
                gather(c + 1, (tile + t) * share, (tile + t + 1) * share)
            norm(c, t)

    mesh = mesh_ref[...].astype(F32) + encoded[...] * (1.0 / math.sqrt(enc))
    hidden_mesh[...] = mesh.astype(BF16)
    qwindow[1 + at.me] = jnp.dot(hidden_mesh[...], wp[...], preferred_element_type=F32).astype(BF16)
    qfetch = Fetch(at, qwindow.at[1 + at.me], qwindow, *fetch_q)
    qfetch.start()
    qfetch.clear()
    receiver[...] = jnp.dot(hidden_mesh[...], wr[...], preferred_element_type=F32)
    count = slots * rows
    mesh_first = at.band * (rows * subs) - rows
    node = lax.broadcasted_iota(jnp.int32, (count, fan * rows), 0)
    picks[...] = jnp.where(node == mv_ref[...] - mesh_first, 1.0, 0.0).astype(BF16)
    qfetch.wait_partner()
    for k in range(1, at.chips):
        qfetch.wait_near(k)
    qfetch.wait_border()
    for k in range(1, at.chips):
        qfetch.wait_far(k)
    qfetch.wait_other_border()
    mesh_before = contract(picks[...], qwindow[...].reshape(count, latent), 0, 0)
    upstream = cot_ref[...].astype(F32)
    scaled = upstream * (1.0 / math.sqrt(fan))
    summed = jnp.zeros((rows, latent), F32)
    received = jnp.zeros((rows, latent), F32)
    for j in range(fan):
        value = mesh_before[j * rows : (j + 1) * rows] + receiver[...]
        active, slope_value = silu_pair(value)
        summed = summed + active
        slope_value = scaled * slope_value
        received = received + slope_value
        mslope[j * rows : (j + 1) * rows] = slope_value.astype(BF16)
    window = jnp.dot(picks[...], mslope[...], preferred_element_type=F32)
    qslots[...] = window.astype(BF16).reshape(slots, rows, latent)
    qreturn = Return(at, qslots, *return_q)
    for s in list(range(1, at.chips)) + [at.chips, 0]:
        qreturn.swap(s)
    mesh_out[...] = (hidden_mesh[...].astype(F32) + summed * (1.0 / math.sqrt(fan))).astype(BF16)
    rgrad[...] = received.astype(BF16)
    for s in range(1, at.chips):
        qreturn.send_across(s)
    qreturn.send_border()
    mgrad[...] = upstream + contract(rgrad[...], wr[...], 1, 1)
    qreturn.total(qgrad)
    upper = mgrad[...] + contract(qgrad[...].astype(BF16), wp[...], 1, 1)
    upper = upper * (1.0 / math.sqrt(enc))
    mgrad[...] = upper
    ugrad[...] = upper - jnp.mean(upper, axis=-1, keepdims=True)

    def decode(k, carry):
        base = pl.multiple_of(k * rows, rows)
        value = normed[pl.ds(base, rows), :].astype(F32)
        both = jnp.mean(mgrad[...] * value, axis=-1, keepdims=True)
        out = (ugrad[...] - value * both) * inverse[pl.ds(base, rows), 0:1]
        grad[pl.ds(base, rows), :] = out.astype(BF16)
        return carry

    lax.fori_loop(0, enc, decode, 0, unroll=8)
    edge_value = contract(act[...], grad[...], 0, 0).astype(BF16)
    edge_v[...] = edge_value.reshape(edge_v.shape)
    edge = Reduce(at, edge_v, edge_out, *scratch_e)
    left = Reduce(at, left_v, src_out.at[:, :, :, 0:half], *scratch_l)
    right = Reduce(at, right_v, src_out.at[:, :, :, half:latent], *scratch_r)
    edge.start()
    back = contract(grad[...], wedge[...], 1, 1) * slope[...].astype(F32)
    bgrad[...] = back.astype(BF16)

    def scatter(h, slot):
        lane = slice(h * half, (h + 1) * half)
        node = lax.broadcasted_iota(jnp.int32, (nodes, enc * rows), 0) + (first + slot * nodes)
        hot = jnp.where(node == gv_ref[...], 1.0, 0.0).astype(BF16)
        total = jnp.dot(hot, bgrad[:, lane], preferred_element_type=F32)
        wgrad[pl.ds(pl.multiple_of(slot * nodes, nodes), nodes), lane] = total.astype(BF16)

    def source(h, ref):
        lane = slice(h * half, (h + 1) * half)
        total = jnp.dot(hid_t[...], wgrad[:, lane], preferred_element_type=F32)
        ref[...] = total.astype(BF16).reshape(ref.shape)

    def grid_back(slot):
        value = contract(wgrad[pl.ds(pl.multiple_of(slot * nodes, nodes), nodes), :], ws[...], 1, 1)
        value = (value * slope_pre[slot].astype(F32)).astype(BF16)
        gslots[slot] = contract(we[...], value, 1, 1).astype(BF16)

    greturn = Return(at, gslots, *return_g)

    def pair(s, work):
        def one(which, carry):
            if s == at.chips:
                slot = which * (subs + 1)
            else:
                slot = 1 + 2 * lax.rem(at.chip + s, at.chips) + which
            work(slot)
            return carry

        lax.fori_loop(0, 2, one, 0)

    def scatter_left(slot, carry):
        scatter(0, slot)
        return carry

    def scatter_right(slot):
        scatter(1, slot)

    edge.to_quarters()
    lax.fori_loop(0, slots, scatter_left, 0)
    edge.to_exchange()
    source(0, left_v)
    left.start()
    pair(at.chips, scatter_right)
    left.to_quarters()
    pair(at.chips, grid_back)
    greturn.swap(at.chips)
    for s in range(1, at.chips):
        pair(s, scatter_right)
    greturn.send_border()
    pair(0, scatter_right)
    left.to_exchange()
    source(1, right_v)
    right.start()
    for s in range(1, at.chips):
        pair(s, grid_back)
        greturn.swap(s)
    right.to_quarters()
    for s in range(1, at.chips):
        greturn.send_across(s)
    pair(0, grid_back)
    greturn.swap(0)
    right.to_exchange()
    edge.to_back()
    left.to_back()
    greturn.total(grid_out)
    right.to_back()
    edge.to_relay()
    left.to_relay()
    right.to_relay()
    for stream in (greturn, qreturn, xfetch, qfetch, edge, left):
        stream.finish()
    edge_full[...] = edge_out[...].astype(F32).reshape(latent, latent)
    src_full[:, 0:half] = src_out[:, :, :, 0:half].astype(F32).reshape(latent, half)
    right.finish()
    src_full[:, half:latent] = src_out[:, :, :, half:latent].astype(F32).reshape(latent, half)


def whole(bands, subs, sizes, channels, args):
    nodes, rows, enc, fan, latent, tile = sizes
    chips, outers, slots = subs // 2, bands // INNER, subs + 2
    edges = rows * enc
    half = latent // 2
    dma = pltpu.SemaphoreType.DMA
    square = pltpu.VMEM((latent, latent), BF16)
    small = pltpu.VMEM((rows, latent), F32)
    small_low = pltpu.VMEM((rows, latent), BF16)
    wide = pltpu.VMEM((edges, latent), BF16)
    scratch = [
        pltpu.VMEM((slots, channels, nodes), BF16),
        pltpu.VMEM((channels, latent), BF16),
        square, square, square, square, square,
        pltpu.VMEM((slots * nodes * latent // LANES, LANES), F32),
        pltpu.VMEM((tile * rows * latent // LANES, LANES), F32),
        pltpu.VMEM((tile * rows * latent // LANES, LANES), F32),
        pltpu.VMEM((latent, slots * nodes), BF16),
        pltpu.VMEM((slots, nodes, latent), BF16),
        small,
        wide, wide, wide,
        pltpu.VMEM((edges, LANES), F32),
        pltpu.VMEM((tile * rows, latent), F32),
        small, small_low, small,
        pltpu.VMEM((slots * rows, fan * rows), BF16),
        pltpu.VMEM((slots, rows, latent), BF16),
        pltpu.VMEM((fan * rows, latent), BF16),
        small_low,
        pltpu.VMEM((slots, rows, latent), BF16),
        small, small, small,
        wide, wide,
        pltpu.VMEM(reduce_shape(chips, latent, latent), BF16),
        pltpu.VMEM((slots * nodes, latent), BF16),
        pltpu.VMEM(reduce_shape(chips, latent, half), BF16),
        pltpu.VMEM(reduce_shape(chips, latent, half), BF16),
        pltpu.VMEM((slots, channels, nodes), BF16),
        pltpu.VMEM(reduce_shape(chips, latent, latent), BF16),
        pltpu.VMEM(reduce_shape(chips, latent, latent), BF16),
        pltpu.VMEM((1, edges), jnp.int32),
        pltpu.VMEM((1, fan * rows), jnp.int32),
        dma((7,)),
    ]
    scratch += fetch_scratch(chips, subs) * 2
    scratch += return_scratch(chips, (rows, latent)) + return_scratch(chips, (channels, nodes))
    scratch += reduce_scratch(chips, outers, latent, latent)
    scratch += reduce_scratch(chips, outers, latent, half) * 2
    return pl.pallas_call(
        functools.partial(whole_kernel, bands, subs, sizes),
        out_shape=[
            pltpu.VMEM((rows, latent), BF16),
            pltpu.VMEM((channels, nodes), F32),
            pltpu.VMEM((latent, latent), F32),
            pltpu.VMEM((latent, latent), F32),
        ],
        in_specs=[ANY, VMEM] + [ANY] * 6 + [SMEM, VMEM, VMEM, VMEM],
        out_specs=[VMEM] * 4,
        scratch_shapes=scratch,
        compiler_params=pltpu.CompilerParams(collective_id=0, has_side_effects=True, vmem_limit_bytes=60 << 20),
        name="whole",
    )(*args)


def finish_kernel(count, *refs):
    ins, outs, sems = refs[:count], refs[count : 2 * count], refs[2 * count]
    copies = [pltpu.make_async_copy(ins[i], outs[i], sems.at[i]) for i in range(count)]
    for copy in copies:
        copy.start()
    for copy in copies:
        copy.wait()


def finish(arrays):
    count = len(arrays)
    return pl.pallas_call(
        functools.partial(finish_kernel, count),
        out_shape=[jax.ShapeDtypeStruct(array.shape, array.dtype) for array in arrays],
        in_specs=[VMEM] * count,
        out_specs=[ANY] * count,
        scratch_shapes=[pltpu.SemaphoreType.DMA((count,))],
        compiler_params=pltpu.CompilerParams(vmem_limit_bytes=1 << 20),
        name="finish",
    )(*arrays)


def body(
    bands, subs,
    grid_x, mesh_in, w_embed, w_src, w_dst, w_edge, w_proc, w_recv, g2m_src, mesh_src, cotangent
):
    latent = w_src.shape[0]
    channels, nodes = grid_x.shape
    rows, enc = g2m_src.shape
    fan = mesh_src.shape[1]
    sizes = (nodes, rows, enc, fan, latent, 4)
    by_edge = g2m_src.T
    args = (
        grid_x, mesh_in, w_embed, w_src, w_dst, w_edge, w_proc, w_recv,
        by_edge, by_edge, mesh_src.T, cotangent,
    )
    return finish(whole(bands, subs, sizes, channels, args))


def solution(mesh):
    nodes = P(("band", "sub"), None)
    placed = (P(None, ("band", "sub")), nodes) + (P(),) * 6 + (nodes,) * 3
    return jax.shard_map(
        functools.partial(body, mesh.shape["band"], mesh.shape["sub"]),
        mesh=mesh,
        in_specs=placed,
        out_specs=(nodes, P(None, ("band", "sub")), P(), P()),
        check_vma=False,
    )
```
